32 devices in a mesh: pr: 4 (over y, x), pc: 8 (over z, core).
Axes of the slice: x: 2, y: 2, z: 4, core: 2. Of those that a mesh axis runs over, the one named last changes fastest.
Arguments:
- pair_state: bfloat16 [96, 96, 128], P('pr', 'pc'), may hold values from -6 to 6
- left_weight: bfloat16 [128, 128], replicated, may hold values from -0.5 to 0.5
- right_weight: bfloat16 [128, 128], replicated, may hold values from -0.5 to 0.5
- mid_gain: float32 [128], replicated, may hold values from 0.25 to 1.75
- out_weight: bfloat16 [128, 128], replicated, may hold values from -0.5 to 0.5
- out_gate: bfloat16 [128, 128], replicated, may hold values from -0.5 to 0.5
Outputs:
- pair_update: bfloat16 [96, 96, 128], P('pr', 'pc')
The draws below stay inside these ranges and needn't reach their ends.
All inputs are finite; a program needn't handle non-finite values.
Results may differ from the reference program's by a relative error of at most 0.012.
Values may be sent and summed in bfloat16 or wider, within the bound.
A program may use at most 128 MiB of HBM per device.

```python
import jax
import jax.numpy as jnp
from jax import lax

RESIDUES = 96
PAIR_WIDTH = 128
MIX_WIDTH = 128


def levels(stream_key, dims, pieces, smallest, top_value):
    level, own = 1.0, jax.random.fold_in(stream_key, 6)
    for dim, shards_of in pieces:
        heights = jnp.exp(jax.random.uniform(jax.random.fold_in(own, dim), (shards_of,), jnp.float32, smallest / len(pieces), top_value / len(pieces)))
        level = level * jnp.repeat(heights, dims[dim] // shards_of).reshape([-1 if axis == dim else 1 for axis in range(len(dims))])
    return level


def scatter_about(key, shape, spread, limit, shards=(), kind=jnp.bfloat16):
    array = spread * jax.random.normal(key, shape, jnp.float32)
    if shards:
        array = array * levels(key, shape, shards, -0.22, 0.18)
    return jnp.clip(array, -limit, limit).astype(kind)


def setup_inputs(seed: int = 0) -> dict:
    keys = jax.random.split(jax.random.key(seed), 7)
    pair_state = scatter_about(keys[0], (RESIDUES, RESIDUES, PAIR_WIDTH), 1.0, 6.0, ((0, 4), (1, 8)))
    left_weight = scatter_about(keys[1], (PAIR_WIDTH, MIX_WIDTH), PAIR_WIDTH ** -0.5, 0.5)
    right_weight = scatter_about(keys[2], (PAIR_WIDTH, MIX_WIDTH), PAIR_WIDTH ** -0.5, 0.5)
    mid_gain = jnp.clip(1.0 + 0.15 * jax.random.normal(keys[3], (MIX_WIDTH,), jnp.float32), 0.25, 1.75)
    out_weight = scatter_about(keys[4], (MIX_WIDTH, PAIR_WIDTH), MIX_WIDTH ** -0.5, 0.5)
    out_gate = scatter_about(keys[5], (PAIR_WIDTH, PAIR_WIDTH), PAIR_WIDTH ** -0.5, 0.5)
    return dict(pair_state=pair_state, left_weight=left_weight, right_weight=right_weight, mid_gain=mid_gain, out_weight=out_weight, out_gate=out_gate)


def scale_channels(values, channel_gain):
    centred = values - lax.optimization_barrier(jnp.mean(values, axis=-1, keepdims=True))
    return centred * lax.rsqrt(lax.optimization_barrier(jnp.mean(centred * centred, axis=-1, keepdims=True)) + 1e-05) * channel_gain

def project_pair(pair_in, left_weight, right_weight):
    ready = pair_in
    left = jnp.einsum('ijc,cd->ijd', ready.astype(jnp.float32), left_weight.astype(jnp.float32))
    right = jnp.einsum('ijc,cd->ijd', ready.astype(jnp.float32), right_weight.astype(jnp.float32))
    return (ready, left.astype(jnp.bfloat16), right.astype(jnp.bfloat16))

def close_update(mixed, ready, mid_gain, out_weight, out_gate):
    scaled = scale_channels(mixed.astype(jnp.float32), mid_gain).astype(jnp.bfloat16)
    scaled = lax.optimization_barrier(scaled)
    gate = jax.nn.sigmoid(jnp.einsum('ijc,cd->ijd', ready.astype(jnp.float32), out_gate.astype(jnp.float32)))
    return (jnp.einsum('ijd,dc->ijc', scaled.astype(jnp.float32), out_weight.astype(jnp.float32)) * gate).astype(jnp.bfloat16)

def reference(pair_state, left_weight, right_weight, mid_gain, out_weight, out_gate):
    ready, left, right = project_pair(pair_state, left_weight, right_weight)
    left, right = lax.optimization_barrier((left, right))

    def one_channel(pair_of):
        return (jnp.dot(pair_of[0].T, pair_of[1], preferred_element_type=jnp.float32) * RESIDUES ** (-0.5)).astype(jnp.bfloat16)
    mixed = jnp.moveaxis(lax.map(one_channel, (jnp.moveaxis(left, -1, 0), jnp.moveaxis(right, -1, 0))), 0, -1)
    mixed = lax.optimization_barrier(mixed)
    return close_update(mixed, ready, mid_gain, out_weight, out_gate)
```

```python
import functools

import jax
import jax.numpy as jnp
from jax import lax
from jax.experimental import pallas as pl
from jax.experimental.pallas import tpu as pltpu
from jax.sharding import PartitionSpec as P

PIECES = 2
MESH = pl.DeviceIdType.MESH


def scale_channels(values, channel_gain):
    centred = values - jnp.mean(values, axis=-1, keepdims=True)
    return (
        centred
        * lax.rsqrt(jnp.mean(centred * centred, axis=-1, keepdims=True) + 1e-05)
        * channel_gain
    )


def project_pair(pair_in, left_weight, right_weight):
    left = jnp.einsum("ijc,cd->ijd", pair_in, left_weight, preferred_element_type=jnp.float32)
    right = jnp.einsum("ijc,cd->ijd", pair_in, right_weight, preferred_element_type=jnp.float32)
    return (pair_in, left.astype(jnp.bfloat16), right.astype(jnp.bfloat16))


def close_update(mixed, ready, mid_gain, out_weight, out_gate):
    scaled = scale_channels(mixed.astype(jnp.float32), mid_gain).astype(jnp.bfloat16)
    scaled = lax.optimization_barrier(scaled)
    gate = jax.nn.sigmoid(
        jnp.einsum("ijc,cd->ijd", ready, out_gate, preferred_element_type=jnp.float32)
    )
    return (
        jnp.einsum("ijd,dc->ijc", scaled, out_weight, preferred_element_type=jnp.float32) * gate
    ).astype(jnp.bfloat16)


def plain_body(pair_state, left_weight, right_weight, mid_gain, out_weight, out_gate):
    ready, left, right = project_pair(pair_state, left_weight, right_weight)
    count = pair_state.shape[0] * lax.axis_size("pr")
    left_lines, right_lines = (
        lax.all_to_all(left, "pr", split_axis=2, concat_axis=0, tiled=True),
        lax.all_to_all(right, "pr", split_axis=2, concat_axis=0, tiled=True),
    )
    strip = jnp.einsum(
        "kid,kjd->ijd",
        lax.all_gather(left_lines, "pc", axis=1, tiled=True),
        right_lines,
        preferred_element_type=jnp.float32,
    )
    strip = (strip * count ** (-0.5)).astype(jnp.bfloat16)
    mixed = lax.all_to_all(strip, "pr", split_axis=0, concat_axis=2, tiled=True)
    return close_update(mixed, ready, mid_gain, out_weight, out_gate)


def kernel(
    rows_of, line_of, J,
    x_hbm, wl_hbm, wr_hbm, gain_hbm, wo_hbm, wg_hbm, o_ref,
    xv, wl, wr, gain, wo, wg, xsib, zbuf, lbuf, rflat, rbuf, flat, mixed, gate, pout, pin,
    in_sem, x_send, x_recv, z_send, z_recv, r_send, p_send, p_recv, ready, ends,
):
    N, D = xv.shape[0] * xv.shape[1], xv.shape[2]
    K = N // J
    G = PIECES
    I = J // G
    part = I * J
    a = lax.axis_index("pr")
    c = lax.axis_index("pc")
    z, core = c // 2, c % 2
    sib = c + 1 - 2 * core
    way = 1 - 2 * (z // 2)
    inner = ((z + 1) % line_of) // 2
    middle = inner == 1
    near = z + way
    far = (z - way + line_of) % line_of
    third = (z + 2) % line_of
    across = a + 1 - 2 * (a % 2)
    along_y = (a + 2) % rows_of

    barrier = pltpu.get_barrier_semaphore()

    def greet(row, column):
        pl.semaphore_signal(barrier, inc=1, device_id=(row, column), device_id_type=MESH)

    greet(a, near * 2 + core)
    pl.when(middle)(lambda: greet(a, far * 2 + core))
    for row in (across, along_y):
        greet(row, c)
        greet(row, sib)
    greet(a, sib)
    loads = [
        pltpu.make_async_copy(s, d, in_sem.at[n])
        for n, (s, d) in enumerate(
            ((x_hbm, xv), (wr_hbm, wr), (wl_hbm, wl), (wg_hbm, wg), (gain_hbm, gain), (wo_hbm, wo))
        )
    ]
    for load in loads:
        load.start()
    for load in loads:
        load.wait()

    xs = xv[...].reshape(N, D)
    own = jnp.dot(xs, wr[...], preferred_element_type=jnp.float32)
    rflat[:N, :] = own
    lbuf[...] = jnp.dot(xs, wl[...], preferred_element_type=jnp.float32)
    gate[...] = jax.nn.sigmoid(jnp.dot(xs, wg[...], preferred_element_type=jnp.float32))

    pl.semaphore_wait(barrier, 6 + inner)

    def along(src, origin, g, target, sem):
        return pltpu.make_async_remote_copy(
            src_ref=src, dst_ref=zbuf.at[origin, g], send_sem=sem, recv_sem=z_recv.at[origin, g],
            device_id=(a, target * 2 + core), device_id_type=MESH,
        )

    def arrived(origin, g):
        pltpu.make_async_copy(xv.at[g], zbuf.at[origin, g], z_recv.at[origin, g]).wait()

    to_sib = pltpu.make_async_remote_copy(
        src_ref=xv, dst_ref=xsib, send_sem=x_send, recv_sem=x_recv,
        device_id=(a, sib), device_id_type=MESH,
    )
    to_sib.start()
    outward = [along(xv.at[g], z, g, far, z_send.at[1, g]) for g in range(G)]
    sent = [along(xv.at[g], z, g, near, z_send.at[0, g]) for g in range(G)]
    for copy in sent:
        copy.start()

    pl.semaphore_signal(ready, inc=1, device_id=(across, c), device_id_type=MESH)

    @pl.when(middle)
    def _():
        pl.semaphore_signal(ends, inc=1, device_id=(a, near * 2 + core), device_id_type=MESH)
        for copy in outward:
            copy.start()
        pl.semaphore_wait(ends, 1)
        pl.semaphore_signal(ends, inc=1, device_id=(a, far * 2 + core), device_id_type=MESH)

    @pl.when(jnp.logical_not(middle))
    def _():
        pl.semaphore_wait(ends, 1)
        for copy in outward:
            copy.start()

    to_sib.wait()
    rflat[N:, :] = jnp.dot(xsib[...].reshape(N, D), wr[...], preferred_element_type=jnp.float32)
    for k in range(K):
        rbuf[k] = rflat[pl.ds(k, 2 * J, stride=K), :]

    sums_sent = []

    def contract(t, origin, g, base):
        def step(k, sums):
            right = rbuf[k]
            return tuple(
                total + lbuf[pl.ds(base + i * K + k, 1), :] * right for i, total in enumerate(sums)
            )

        sums = lax.fori_loop(
            0, K, step, tuple(jnp.zeros((2 * J, D), jnp.float32) for _ in range(I)), unroll=K
        )
        for i in range(I):
            flat[i * J : (i + 1) * J, :] = sums[i][:J]
        pout[t, g, 0] = flat[:part, :].astype(pout.dtype)
        landing, sem = pin.at[g, core, a], p_recv.at[g, core, a]
        away = pltpu.make_async_remote_copy(
            src_ref=pout.at[t, g, 0], dst_ref=landing, send_sem=p_send.at[t, g, 0], recv_sem=sem,
            device_id=(origin, c), device_id_type=MESH,
        )
        here = pltpu.make_async_copy(pout.at[t, g, 0], landing, sem)
        side = pltpu.make_async_remote_copy(
            src_ref=pout.at[t, g, 1], dst_ref=landing, send_sem=p_send.at[t, g, 1], recv_sem=sem,
            device_id=(origin, sib), device_id_type=MESH,
        )
        pl.when(origin != a)(away.start)
        pl.when(origin == a)(here.start)
        for i in range(I):
            flat[part + i * J : part + (i + 1) * J, :] = sums[i][J:]
        pout[t, g, 1] = flat[part:, :].astype(pout.dtype)
        side.start()
        sums_sent.append((origin, away, side))

    def project(origin, g):
        block = zbuf[origin, g]
        lbuf[: I * K, :] = jnp.dot(block, wl[...], preferred_element_type=jnp.float32)

    pl.semaphore_wait(ready, 1)
    for g in range(G):
        contract(0, z, g, g * I * K)
    relays = []
    for g in range(G):
        arrived(near, g)
        first = along(zbuf.at[near, g], near, g, far, r_send.at[0, g])
        second = along(zbuf.at[far, g], far, g, near, r_send.at[1, g])
        relays += [first, second]

        @pl.when(middle)
        def _():
            first.start()
            arrived(far, g)
            second.start()

    for g in range(G):
        project(near, g)
        contract(1, near, g, 0)
    for g in range(G):

        @pl.when(jnp.logical_not(middle))
        def _():
            arrived(far, g)

        project(far, g)
        contract(2, far, g, 0)
        arrived(third, g)
        project(third, g)
        contract(3, third, g, 0)

    for g in range(G):
        totals = []
        for s in range(2):
            for row in range(rows_of):
                pltpu.make_async_copy(pout.at[0, 0, 0], pin.at[g, s, row], p_recv.at[g, s, row]).wait()
            total = pin[g, s, 0].astype(jnp.float32)
            for row in range(1, rows_of):
                total += pin[g, s, row].astype(jnp.float32)
            totals.append(total)
        total = jnp.concatenate(totals, axis=0) * (K * rows_of) ** (-0.5)
        total = total.astype(jnp.bfloat16).astype(jnp.float32)
        scaled = scale_channels(total, gain[...]).astype(jnp.bfloat16)
        out = jnp.dot(scaled, wo[...], preferred_element_type=jnp.float32)
        for s in range(2):
            for i in range(I):
                first_row = s * part + i * J
                mixed[pl.ds((s * G + g) * I + i, J, stride=K), :] = out[first_row : first_row + J]
    o_ref[...] = (mixed[...] * gate[...]).astype(o_ref.dtype)

    for copy in sent:
        copy.wait_send()

    for copy in outward:
        copy.wait_send()

    @pl.when(middle)
    def _():
        for copy in relays:
            copy.wait_send()

    for origin, away, side in sums_sent:
        pl.when(origin != a)(away.wait_send)
        side.wait_send()


def kernel_body(rows_of, line_of, pair_state, left_weight, right_weight, mid_gain, out_weight, out_gate):
    K, J, D = pair_state.shape
    N = K * J
    G = PIECES
    I = J // G
    f32, bf16 = jnp.float32, jnp.bfloat16
    anywhere = pl.BlockSpec(memory_space=pl.ANY)
    dma = pltpu.SemaphoreType.DMA
    pieces = jnp.transpose(pair_state, (1, 0, 2)).reshape(G, I * K, D)
    update = pl.pallas_call(
        functools.partial(kernel, rows_of, line_of, J),
        out_shape=pltpu.VMEM((N, D), bf16),
        in_specs=[anywhere] * 6,
        out_specs=pl.BlockSpec(memory_space=pltpu.VMEM),
        scratch_shapes=[
            pltpu.VMEM((G, I * K, D), bf16),
            pltpu.VMEM((D, D), bf16),
            pltpu.VMEM((D, D), bf16),
            pltpu.VMEM((1, D), f32),
            pltpu.VMEM((D, D), bf16),
            pltpu.VMEM((D, D), bf16),
            pltpu.VMEM((G, I * K, D), bf16),
            pltpu.VMEM((line_of, G, I * K, D), bf16),
            pltpu.VMEM((N, D), f32),
            pltpu.VMEM((2 * N, D), f32),
            pltpu.VMEM((K, 2 * J, D), f32),
            pltpu.VMEM((2 * I * J, D), f32),
            pltpu.VMEM((N, D), f32),
            pltpu.VMEM((N, D), f32),
            pltpu.VMEM((line_of, G, 2, I * J, D), bf16),
            pltpu.VMEM((G, 2, rows_of, I * J, D), bf16),
            dma((6,)), dma, dma, dma((2, G)), dma((line_of, G)), dma((2, G)),
            dma((line_of, G, 2)), dma((G, 2, rows_of)), pltpu.SemaphoreType.REGULAR,
            pltpu.SemaphoreType.REGULAR,
        ],
        compiler_params=pltpu.CompilerParams(collective_id=0, has_side_effects=True),
    )(pieces, left_weight, right_weight, mid_gain.reshape(1, -1), out_weight, out_gate)
    return jnp.transpose(update.reshape(J, K, D), (1, 0, 2))


def body(rows_of, columns_of, *arrays):
    K, J, D = arrays[0].shape
    fits = (
        columns_of == 2 * rows_of
        and columns_of == 8
        and K == 2 * J
        and arrays[1].shape == (D, D)
        and D % 128 == 0
        and J <= 16
        and J % PIECES == 0
    )
    if fits:
        return kernel_body(rows_of, columns_of // 2, *arrays)
    return plain_body(*arrays)


def solution(mesh):
    placed = (P("pr", "pc", None), P(), P(), P(), P(), P())
    return jax.shard_map(
        functools.partial(body, mesh.shape["pr"], mesh.shape["pc"]),
        mesh=mesh, in_specs=placed, out_specs=P("pr", "pc", None), check_vma=False,
    )
```

```python
import functools

import jax
import jax.numpy as jnp
from jax import lax
from jax.experimental import pallas as pl
from jax.experimental.pallas import tpu as pltpu
from jax.sharding import PartitionSpec as P

PIECES = 3
MESH = pl.DeviceIdType.MESH


def whole(*chips):
    return tuple((chip, g) for chip in chips for g in range(PIECES))


def mixed(*chips):
    return tuple((chip, g) for g in range(PIECES) for chip in chips)


DOWN = (((), whole(0), whole(0, 1), mixed(0, 2, 1)), ((), whole(0), whole(1), mixed(0, 2, 1)))
UP = ((whole(1), whole(2), whole(3), ()), (whole(1), whole(2), whole(3), ()))
LATER = ((mixed(2, 3), whole(3), (), ()), (mixed(2, 3), (), (), ()))
ORDER = ((whole(1) + mixed(3, 2), mixed(0, 2, 3), mixed(1, 3, 0), whole(2) + mixed(1, 0)), (whole(1) + mixed(2, 3), mixed(0, 2, 3), mixed(3, 0, 1), whole(2) + mixed(0, 1)))


def scale_channels(values, channel_gain):
    centred = values - jnp.mean(values, axis=-1, keepdims=True)
    return (
        centred
        * lax.rsqrt(jnp.mean(centred * centred, axis=-1, keepdims=True) + 1e-05)
        * channel_gain
    )


def project_pair(pair_in, left_weight, right_weight):
    left = jnp.einsum("ijc,cd->ijd", pair_in, left_weight, preferred_element_type=jnp.float32)
    right = jnp.einsum("ijc,cd->ijd", pair_in, right_weight, preferred_element_type=jnp.float32)
    return (pair_in, left.astype(jnp.bfloat16), right.astype(jnp.bfloat16))


def close_update(mixed, ready, mid_gain, out_weight, out_gate):
    scaled = scale_channels(mixed.astype(jnp.float32), mid_gain).astype(jnp.bfloat16)
    scaled = lax.optimization_barrier(scaled)
    gate = jax.nn.sigmoid(
        jnp.einsum("ijc,cd->ijd", ready, out_gate, preferred_element_type=jnp.float32)
    )
    return (
        jnp.einsum("ijd,dc->ijc", scaled, out_weight, preferred_element_type=jnp.float32) * gate
    ).astype(jnp.bfloat16)


def plain_body(pair_state, left_weight, right_weight, mid_gain, out_weight, out_gate):
    ready, left, right = project_pair(pair_state, left_weight, right_weight)
    count = pair_state.shape[0] * lax.axis_size("pr")
    left_lines, right_lines = (
        lax.all_to_all(left, "pr", split_axis=2, concat_axis=0, tiled=True),
        lax.all_to_all(right, "pr", split_axis=2, concat_axis=0, tiled=True),
    )
    strip = jnp.einsum(
        "kid,kjd->ijd",
        lax.all_gather(left_lines, "pc", axis=1, tiled=True),
        right_lines,
        preferred_element_type=jnp.float32,
    )
    strip = (strip * count ** (-0.5)).astype(jnp.bfloat16)
    mixed = lax.all_to_all(strip, "pr", split_axis=0, concat_axis=2, tiled=True)
    return close_update(mixed, ready, mid_gain, out_weight, out_gate)


def kernel(
    rows_of, line_of, J,
    x_hbm, wl_hbm, wr_hbm, gain_hbm, wo_hbm, wg_hbm, o_ref,
    xv, wl, wr, gain, wo, wg, xsib, lv, zbuf, lbuf, rflat, rbuf, flat, merged, gate, pout, pin,
    in_sem, x_send, x_recv, z_send, z_recv, r_send, p_send, p_recv, ready, risen,
):
    N, D = xv.shape[0] * xv.shape[1], xv.shape[2]
    K = N // J
    G = PIECES
    I = J // G
    part = I * J
    last = line_of - 1
    a = lax.axis_index("pr")
    c = lax.axis_index("pc")
    z, core = c // 2, c % 2
    other = 1 - core
    sib = 2 * z + other
    p, q = a % 2, a // 2
    across, along_y, opposite = a + 1 - 2 * p, (a + 2) % rows_of, rows_of - 1 - a
    inner = ((z + 1) % line_of) // 2
    relaying = inner * core

    barrier = pltpu.get_barrier_semaphore()

    def tell(semaphore, row, column):
        pl.semaphore_signal(semaphore, inc=1, device_id=(row, column), device_id_type=MESH)

    def tell_chip(semaphore, row):
        tell(semaphore, row, c)
        tell(semaphore, row, sib)

    loads = [
        pltpu.make_async_copy(s, d, in_sem.at[n])
        for n, (s, d) in enumerate(
            ((x_hbm, xv), (wl_hbm, wl), (wr_hbm, wr), (wg_hbm, wg), (gain_hbm, gain), (wo_hbm, wo))
        )
    ]
    for load in loads:
        load.start()

    tell(barrier, a, sib)
    for level in range(1, line_of):

        @pl.when(z < level)
        def _():
            tell(barrier, a, 2 * level)
            tell(barrier, a, 2 * level + 1)

    pl.when(p == 0)(lambda: tell_chip(barrier, across))
    pl.when(q == 0)(lambda: tell_chip(barrier, along_y))
    pl.when(a == 0)(lambda: tell_chip(barrier, opposite))

    routes = [[sorted({chip for chip, g in DOWN[h][l] + UP[h][l] + LATER[h][l]}) for l in range(line_of)] for h in range(2)]

    def along(src, origin, half, g, column, sem):
        return pltpu.make_async_remote_copy(
            src_ref=src, dst_ref=zbuf.at[origin, half, g], send_sem=sem,
            recv_sem=z_recv.at[origin, half, g], device_id=(a, column), device_id_type=MESH,
        )

    def flow(half, level, target, g):
        between = 0 < level < last and 0 < target < last
        column = 2 * target + (1 if between else 1 - half)
        slot = routes[half][level].index(target)
        return along(lv.at[g], level, half, g, column, z_send.at[slot, g])

    def everywhere(act):
        for half in range(2):
            for level in range(line_of):
                if act.keywords["plan"][half][level]:
                    pl.when(jnp.logical_and(z == level, core == half))(functools.partial(act, half, level))

    def launch(half, level, plan):
        risen_to = level
        for target, g in plan[half][level]:
            if target > risen_to:
                for higher in range(risen_to + 1, target + 1):
                    if higher in [chip for chip, _ in plan[half][level]]:
                        pl.semaphore_wait(risen.at[higher], 2)
                risen_to = target
            flow(half, level, target, g).start()

    def arrived(origin, half, g):
        pltpu.make_async_copy(xv.at[0], zbuf.at[origin, half, g], z_recv.at[origin, half, g]).wait()

    to_sib = pltpu.make_async_remote_copy(
        src_ref=xv, dst_ref=xsib, send_sem=x_send, recv_sem=x_recv,
        device_id=(a, sib), device_id_type=MESH,
    )

    pl.semaphore_wait(barrier, 1 + 2 * z + 2 * (p + q + p * q))
    for level in range(1, line_of):

        @pl.when(z == level)
        def _():
            for half in range(2):
                for lower in (low for low in range(level) if level in routes[half][low]):
                    tell(risen.at[level], a, 2 * lower + half)

    pl.when(p == 1)(lambda: tell_chip(ready, across))
    pl.when(q == 1)(lambda: tell_chip(ready, along_y))
    pl.when(a == rows_of - 1)(lambda: tell_chip(ready, opposite))

    for load in loads[:2]:
        load.wait()
    to_sib.start()
    for g in range(G):
        rows = slice(g * I * K, (g + 1) * I * K)
        left = jnp.dot(xv[g], wl[...], preferred_element_type=jnp.float32)
        lbuf[rows, :] = left
        lv[g] = left.astype(lv.dtype)
    everywhere(functools.partial(launch, plan=DOWN))

    for load in loads[2:]:
        load.wait()
    xs = xv[...].reshape(N, D)
    rflat[:N, :] = jnp.dot(xs, wr[...], preferred_element_type=jnp.float32)
    gate[...] = jax.nn.sigmoid(jnp.dot(xs, wg[...], preferred_element_type=jnp.float32))

    everywhere(functools.partial(launch, plan=UP))
    to_sib.wait()
    rflat[N:, :] = jnp.dot(xsib[...].reshape(N, D), wr[...], preferred_element_type=jnp.float32)
    for k in range(K):
        rbuf[k] = rflat[pl.ds(k, 2 * J, stride=K), :]
    sums_sent = []

    def contract(t, origin, half, g, base):
        def step(k, sums):
            right = rbuf[k]
            return tuple(
                total + lbuf[pl.ds(base + i * K + k, 1), :] * right for i, total in enumerate(sums)
            )

        sums = lax.fori_loop(
            0, K, step, tuple(jnp.zeros((2 * J, D), jnp.float32) for _ in range(I)), unroll=K
        )
        landing, sem = pin.at[g, half, a], p_recv.at[g, half, a]
        away = pltpu.make_async_remote_copy(
            src_ref=pout.at[t, 0], dst_ref=landing, send_sem=p_send.at[t, 0], recv_sem=sem,
            device_id=(origin, c), device_id_type=MESH,
        )
        stay = pltpu.make_async_copy(pout.at[t, 0], landing, sem)
        side = pltpu.make_async_remote_copy(
            src_ref=pout.at[t, 1], dst_ref=landing, send_sem=p_send.at[t, 1], recv_sem=sem,
            device_id=(origin, sib), device_id_type=MESH,
        )
        for i in range(I):
            flat[i * J : (i + 1) * J, :] = sums[i][:J]
            flat[part + i * J : part + (i + 1) * J, :] = sums[i][J:]
        pout[t, 0] = flat[:part, :].astype(pout.dtype)
        pl.when(origin != a)(away.start)
        pl.when(origin == a)(stay.start)
        pout[t, 1] = flat[part:, :].astype(pout.dtype)
        side.start()
        sums_sent.append((origin, away, side))

    @pl.when(a < rows_of - 1)
    def _():
        pl.semaphore_wait(ready, 2 * ((1 - p) + (1 - q) + (1 - p) * (1 - q)))

    for g in range(G):
        contract(g, z, core, g, g * I * K)

    everywhere(functools.partial(launch, plan=LATER))

    peer = last - z
    outer = (peer + 2) % line_of
    relays = []
    for g in range(G):
        held = zbuf.at[peer, 1, g]
        relays.append(along(held, peer, 1, g, 2 * outer, r_send.at[0, g]))
        relays.append(along(held, peer, 1, g, sib, r_send.at[1, g]))

    @pl.when(relaying == 1)
    def _():
        for g in range(G):
            arrived(peer, 1, g)
            for copy in relays[2 * g : 2 * g + 2]:
                copy.start()

    def at_level(values):
        picked = values[0]
        for level in range(1, line_of):
            picked = picked + (z // level) * (1 - z // (level + 1)) * (values[level] - values[0])
        return picked

    def pick(lower, upper):
        return lower + core * (upper - lower)

    for n in range(last * G):
        origin, g = (
            pick(*(at_level([ORDER[half][level][n][e] for level in range(line_of)]) for half in range(2)))
            for e in range(2)
        )
        arrived(origin, other, g)
        lbuf[: I * K, :] = zbuf[origin, other, g].astype(jnp.float32)
        contract(G + n, origin, other, g, 0)

    for g in range(G):
        for s in range(2):
            for row in range(rows_of):
                pltpu.make_async_copy(pout.at[0, 0], pin.at[g, s, row], p_recv.at[g, s, row]).wait()
    for g in range(G):
        totals = []
        for s in range(2):
            total = pin[g, s, 0].astype(jnp.float32)
            for row in range(1, rows_of):
                total += pin[g, s, row].astype(jnp.float32)
            totals.append(total)
        total = jnp.concatenate(totals, axis=0) * (K * rows_of) ** (-0.5)
        total = total.astype(jnp.bfloat16).astype(jnp.float32)
        scaled = scale_channels(total, gain[...]).astype(jnp.bfloat16)
        out = jnp.dot(scaled, wo[...], preferred_element_type=jnp.float32)
        for s in range(2):
            for i in range(I):
                first_row = s * part + i * J
                merged[pl.ds((s * G + g) * I + i, J, stride=K), :] = out[first_row : first_row + J]
    o_ref[...] = (merged[...] * gate[...]).astype(o_ref.dtype)

    def settle(half, level, plan):
        for target in plan[half][level]:
            for g in range(G):
                flow(half, level, target, g).wait_send()

    everywhere(functools.partial(settle, plan=routes))

    @pl.when(relaying == 1)
    def _():
        for copy in relays:
            copy.wait_send()

    for origin, away, side in sums_sent:
        pl.when(origin != a)(away.wait_send)
        side.wait_send()


def kernel_body(rows_of, line_of, pair_state, left_weight, right_weight, mid_gain, out_weight, out_gate):
    K, J, D = pair_state.shape
    N = K * J
    G = PIECES
    I = J // G
    f32, bf16 = jnp.float32, jnp.bfloat16
    anywhere = pl.BlockSpec(memory_space=pl.ANY)
    dma = pltpu.SemaphoreType.DMA
    pieces = jnp.transpose(pair_state, (1, 0, 2)).reshape(G, I * K, D)
    update = pl.pallas_call(
        functools.partial(kernel, rows_of, line_of, J),
        out_shape=pltpu.VMEM((N, D), bf16),
        in_specs=[anywhere] * 6,
        out_specs=pl.BlockSpec(memory_space=pltpu.VMEM),
        scratch_shapes=[
            pltpu.VMEM((G, I * K, D), bf16),
            pltpu.VMEM((D, D), bf16),
            pltpu.VMEM((D, D), bf16),
            pltpu.VMEM((1, D), f32),
            pltpu.VMEM((D, D), bf16),
            pltpu.VMEM((D, D), bf16),
            pltpu.VMEM((G, I * K, D), bf16),
            pltpu.VMEM((G, I * K, D), bf16),
            pltpu.VMEM((line_of, 2, G, I * K, D), bf16),
            pltpu.VMEM((N, D), f32),
            pltpu.VMEM((2 * N, D), f32),
            pltpu.VMEM((K, 2 * J, D), f32),
            pltpu.VMEM((2 * I * J, D), f32),
            pltpu.VMEM((N, D), f32),
            pltpu.VMEM((N, D), f32),
            pltpu.VMEM((line_of * G, 2, I * J, D), bf16),
            pltpu.VMEM((G, 2, rows_of, I * J, D), bf16),
            dma((6,)), dma, dma, dma((3, G)), dma((line_of, 2, G)), dma((2, G)),
            dma((line_of * G, 2)), dma((G, 2, rows_of)), pltpu.SemaphoreType.REGULAR,
            pltpu.SemaphoreType.REGULAR((line_of,)),
        ],
        compiler_params=pltpu.CompilerParams(collective_id=0, has_side_effects=True),
    )(pieces, left_weight, right_weight, mid_gain.reshape(1, -1), out_weight, out_gate)
    return jnp.transpose(update.reshape(J, K, D), (1, 0, 2))


def body(rows_of, columns_of, *arrays):
    K, J, D = arrays[0].shape
    fits = (
        columns_of == 2 * rows_of
        and columns_of == 8
        and K == 2 * J
        and arrays[1].shape == (D, D)
        and D % 128 == 0
        and J <= 16
        and J % PIECES == 0
    )
    if fits:
        return kernel_body(rows_of, columns_of // 2, *arrays)
    return plain_body(*arrays)


def solution(mesh):
    placed = (P("pr", "pc", None), P(), P(), P(), P(), P())
    return jax.shard_map(
        functools.partial(body, mesh.shape["pr"], mesh.shape["pc"]),
        mesh=mesh, in_specs=placed, out_specs=P("pr", "pc", None), check_vma=False,
    )
```

```python
import functools

import jax
import jax.numpy as jnp
from jax import lax
from jax.experimental import pallas as pl
from jax.experimental.pallas import tpu as pltpu
from jax.sharding import PartitionSpec as P

PIECES = 3
MESH = pl.DeviceIdType.MESH


def whole(*chips):
    return tuple((chip, g) for chip in chips for g in range(PIECES))


def mixed(*chips):
    return tuple((chip, g) for g in range(PIECES) for chip in chips)


DOWN = (((), whole(0), whole(0, 1), mixed(0, 2, 1)), ((), whole(0), whole(1), mixed(0, 2, 1)))
UP = ((whole(1), whole(2), whole(3), ()), (whole(1), whole(2), whole(3), ()))
LATER = ((mixed(2, 3), whole(3), (), ()), (mixed(2, 3), (), (), ()))
ORDER = ((whole(1) + mixed(3, 2), whole(0) + mixed(2, 3), whole(1) + mixed(3, 0), whole(2) + mixed(1, 0)), (whole(1) + mixed(2, 3), whole(0) + mixed(2, 3), mixed(3, 0) + whole(1), whole(2) + mixed(0, 1)))


def scale_channels(values, channel_gain):
    centred = values - jnp.mean(values, axis=-1, keepdims=True)
    return (
        centred
        * lax.rsqrt(jnp.mean(centred * centred, axis=-1, keepdims=True) + 1e-05)
        * channel_gain
    )


def project_pair(pair_in, left_weight, right_weight):
    left = jnp.einsum("ijc,cd->ijd", pair_in, left_weight, preferred_element_type=jnp.float32)
    right = jnp.einsum("ijc,cd->ijd", pair_in, right_weight, preferred_element_type=jnp.float32)
    return (pair_in, left.astype(jnp.bfloat16), right.astype(jnp.bfloat16))


def close_update(mixed, ready, mid_gain, out_weight, out_gate):
    scaled = scale_channels(mixed.astype(jnp.float32), mid_gain).astype(jnp.bfloat16)
    scaled = lax.optimization_barrier(scaled)
    gate = jax.nn.sigmoid(
        jnp.einsum("ijc,cd->ijd", ready, out_gate, preferred_element_type=jnp.float32)
    )
    return (
        jnp.einsum("ijd,dc->ijc", scaled, out_weight, preferred_element_type=jnp.float32) * gate
    ).astype(jnp.bfloat16)


def plain_body(pair_state, left_weight, right_weight, mid_gain, out_weight, out_gate):
    ready, left, right = project_pair(pair_state, left_weight, right_weight)
    count = pair_state.shape[0] * lax.axis_size("pr")
    left_lines, right_lines = (
        lax.all_to_all(left, "pr", split_axis=2, concat_axis=0, tiled=True),
        lax.all_to_all(right, "pr", split_axis=2, concat_axis=0, tiled=True),
    )
    strip = jnp.einsum(
        "kid,kjd->ijd",
        lax.all_gather(left_lines, "pc", axis=1, tiled=True),
        right_lines,
        preferred_element_type=jnp.float32,
    )
    strip = (strip * count ** (-0.5)).astype(jnp.bfloat16)
    mixed = lax.all_to_all(strip, "pr", split_axis=0, concat_axis=2, tiled=True)
    return close_update(mixed, ready, mid_gain, out_weight, out_gate)


def kernel(
    rows_of, line_of, J,
    x_hbm, wl_hbm, wr_hbm, gain_hbm, wo_hbm, wg_hbm, o_ref,
    xv, weights, gain, xsib, lv, zbuf, lbuf, rflat, rbuf, flat, merged, gate, pout, pin,
    x_in, weights_in, gain_in, x_recv, z_sent, z_recv, p_sent, p_recv, ready, risen,
):
    N, D = xv.shape[0] * xv.shape[1], xv.shape[2]
    K = N // J
    G = PIECES
    I = J // G
    part = I * J
    last = line_of - 1
    a = lax.axis_index("pr")
    c = lax.axis_index("pc")
    z, core = c // 2, c % 2
    other = 1 - core
    sib = 2 * z + other
    p, q = a % 2, a // 2
    across, along_y, opposite = a + 1 - 2 * p, (a + 2) % rows_of, rows_of - 1 - a
    inner = ((z + 1) % line_of) // 2
    relaying = inner * core

    barrier = pltpu.get_barrier_semaphore()

    def tell(semaphore, row, column):
        pl.semaphore_signal(semaphore, inc=1, device_id=(row, column), device_id_type=MESH)

    def tell_chip(semaphore, row):
        tell(semaphore, row, c)
        tell(semaphore, row, sib)

    load = pltpu.make_async_copy(x_hbm, xv, x_in)
    load.start()
    for n, weight in enumerate((wl_hbm, wr_hbm, wg_hbm, wo_hbm)):
        pltpu.make_async_copy(weight, weights.at[n], weights_in).start()
    load_gain = pltpu.make_async_copy(gain_hbm, gain, gain_in)
    load_gain.start()

    tell(barrier, a, sib)
    for level in range(1, line_of):

        @pl.when(z < level)
        def _():
            tell(barrier, a, 2 * level)
            tell(barrier, a, 2 * level + 1)

    pl.when(p == 0)(lambda: tell_chip(barrier, across))
    pl.when(q == 0)(lambda: tell_chip(barrier, along_y))
    pl.when(a == 0)(lambda: tell_chip(barrier, opposite))

    routes = [
        [sorted({chip for chip, g in DOWN[h][l] + UP[h][l] + LATER[h][l]}) for l in range(line_of)]
        for h in range(2)
    ]

    def place(origin, half, g):
        return zbuf.at[(origin * 2 + half) * G + g]

    def along(src, origin, half, g, column, slot):
        return pltpu.make_async_remote_copy(
            src_ref=src, dst_ref=place(origin, half, g), send_sem=z_sent,
            recv_sem=z_recv.at[slot], device_id=(a, column), device_id_type=MESH,
        )

    def flow(half, level, target, g):
        held = half == 1 and 0 < level < last and 0 < target < last
        column = 2 * target + (1 if held else 1 - half)
        slot = (last if held else (level - target - 1) % line_of) * G + g
        return along(lv.at[g], level, half, g, column, slot)

    def everywhere(act):
        for half in range(2):
            for level in range(line_of):
                if act.keywords["plan"][half][level]:
                    pl.when(jnp.logical_and(z == level, core == half))(functools.partial(act, half, level))

    def launch(half, level, plan, ready_to=None):
        sends = plan[half][level]
        if ready_to is not None:
            ends = [next((n for n, s in enumerate(sends) if s[1] > g), len(sends)) for g in range(-1, G)]
            sends = sends[ends[ready_to] : ends[ready_to + 1]]
        seen = level
        for target, g in sends:
            if target > seen:
                for higher in sorted({chip for chip, _ in sends if seen < chip <= target}):
                    pl.semaphore_wait(risen.at[higher - 1], 2)
                seen = target
            flow(half, level, target, g).start()

    def arrived(origin, half, g, slot):
        pltpu.make_async_copy(xv.at[0], place(origin, half, g), z_recv.at[slot]).wait()

    to_sib = pltpu.make_async_remote_copy(
        src_ref=xv, dst_ref=xsib, send_sem=z_sent, recv_sem=x_recv,
        device_id=(a, sib), device_id_type=MESH,
    )

    pl.semaphore_wait(barrier, 1 + 2 * z + 2 * (p + q + p * q))
    for level in range(1, line_of):

        @pl.when(z == level)
        def _():
            for half in range(2):
                for lower in (low for low in range(level) if level in routes[half][low]):
                    tell(risen.at[level - 1], a, 2 * lower + half)

    pl.when(p == 1)(lambda: tell_chip(ready, across))
    pl.when(q == 1)(lambda: tell_chip(ready, along_y))
    pl.when(a == rows_of - 1)(lambda: tell_chip(ready, opposite))

    load.wait()
    to_sib.start()
    pltpu.make_async_copy(weights, weights, weights_in).wait()
    for g in range(G):
        rows = slice(g * I * K, (g + 1) * I * K)
        left = jnp.dot(xv[g], weights[0], preferred_element_type=jnp.float32)
        lv[g] = left.astype(lv.dtype)
        everywhere(functools.partial(launch, plan=DOWN, ready_to=g))
        lbuf[rows, :] = left

    load_gain.wait()
    xs = xv[...].reshape(N, D)
    rflat[:N, :] = jnp.dot(xs, weights[1], preferred_element_type=jnp.float32)
    gate[...] = jax.nn.sigmoid(jnp.dot(xs, weights[2], preferred_element_type=jnp.float32))

    everywhere(functools.partial(launch, plan=UP))
    to_sib.wait_recv()
    rflat[N:, :] = jnp.dot(xsib[...].reshape(N, D), weights[1], preferred_element_type=jnp.float32)
    for k in range(K):
        rbuf[k] = rflat[pl.ds(k, 2 * J, stride=K), :]


    def contract(t, origin, half, g, base):
        def step(k, sums):
            right = rbuf[k]
            return tuple(
                total + lbuf[pl.ds(base + i * K + k, 1), :] * right for i, total in enumerate(sums)
            )

        sums = lax.fori_loop(
            0, K, step, tuple(jnp.zeros((2 * J, D), jnp.float32) for _ in range(I)), unroll=K
        )
        landing, sem = pin.at[g, half, a], p_recv.at[g]
        away = pltpu.make_async_remote_copy(
            src_ref=pout.at[2 * t], dst_ref=landing, send_sem=p_sent, recv_sem=sem,
            device_id=(origin, c), device_id_type=MESH,
        )
        stay = pltpu.make_async_copy(pout.at[2 * t], landing, sem)
        side = pltpu.make_async_remote_copy(
            src_ref=pout.at[2 * t + 1], dst_ref=landing, send_sem=p_sent, recv_sem=sem,
            device_id=(origin, sib), device_id_type=MESH,
        )
        for i in range(I):
            flat[i * J : (i + 1) * J, :] = sums[i][:J]
            flat[part + i * J : part + (i + 1) * J, :] = sums[i][J:]
        pout[2 * t] = flat[:part, :].astype(pout.dtype)
        pl.when(origin != a)(away.start)
        pl.when(origin == a)(stay.start)
        pout[2 * t + 1] = flat[part:, :].astype(pout.dtype)
        side.start()

    @pl.when(a < rows_of - 1)
    def _():
        pl.semaphore_wait(ready, 2 * ((1 - p) + (1 - q) + (1 - p) * (1 - q)))

    for g in range(G):
        contract(g, z, core, g, g * I * K)

    everywhere(functools.partial(launch, plan=LATER))

    peer = last - z
    outer = (peer + 2) % line_of
    relays = []
    for g in range(G):
        held = place(peer, 1, g)
        relays.append(along(held, peer, 1, g, 2 * outer, G + g))
        relays.append(along(held, peer, 1, g, sib, (peer - z + last) % line_of * G + g))

    @pl.when(relaying == 1)
    def _():
        for g in range(G):
            arrived(peer, 1, g, last * G + g)
            for copy in relays[2 * g : 2 * g + 2]:
                copy.start()

    def at_level(values):
        picked = values[0]
        for level in range(1, line_of):
            picked = picked + (z // level) * (1 - z // (level + 1)) * (values[level] - values[0])
        return picked

    def pick(lower, upper):
        return lower + core * (upper - lower)

    for n in range(last * G):
        origin, g = (
            pick(*(at_level([ORDER[half][level][n][e] for level in range(line_of)]) for half in range(2)))
            for e in range(2)
        )
        arrived(origin, other, g, (origin - z + last) % line_of * G + g)
        lbuf[: I * K, :] = zbuf[(origin * 2 + other) * G + g].astype(jnp.float32)
        contract(G + n, origin, other, g, 0)

    for g in range(G):
        pltpu.make_async_copy(pin.at[g], pin.at[g], p_recv.at[g]).wait()
        totals = []
        for s in range(2):
            total = pin[g, s, 0].astype(jnp.float32)
            for row in range(1, rows_of):
                total += pin[g, s, row].astype(jnp.float32)
            totals.append(total)
        total = jnp.concatenate(totals, axis=0) * (K * rows_of) ** (-0.5)
        total = total.astype(jnp.bfloat16).astype(jnp.float32)
        scaled = scale_channels(total, gain[...]).astype(jnp.bfloat16)
        out = jnp.dot(scaled, weights[3], preferred_element_type=jnp.float32)
        for s in range(2):
            for i in range(I):
                first_row = s * part + i * J
                merged[pl.ds((s * G + g) * I + i, J, stride=K), :] = out[first_row : first_row + J]
    o_ref[...] = (merged[...] * gate[...]).astype(o_ref.dtype)

    def settle(half, level, plan):
        sends = (len(plan[half][level]) + 1) * G
        held = [s for s in plan[half][level] if half == 1 and 0 < level < last and 0 < s < last]
        sent = zbuf.at[pl.ds(0, sends + 2 * G * len(held))]
        pltpu.make_async_copy(sent, sent, z_sent).wait()

    everywhere(functools.partial(settle, plan=routes))
    sent = pout.at[pl.ds(0, (2 * line_of - 1) * G)]
    pltpu.make_async_copy(sent, sent, p_sent).wait()


def kernel_body(rows_of, line_of, pair_state, left_weight, right_weight, mid_gain, out_weight, out_gate):
    K, J, D = pair_state.shape
    N = K * J
    G = PIECES
    I = J // G
    f32, bf16 = jnp.float32, jnp.bfloat16
    anywhere = pl.BlockSpec(memory_space=pl.ANY)
    dma = pltpu.SemaphoreType.DMA
    pieces = jnp.transpose(pair_state, (1, 0, 2)).reshape(G, I * K, D)
    update = pl.pallas_call(
        functools.partial(kernel, rows_of, line_of, J),
        out_shape=pltpu.VMEM((N, D), bf16),
        in_specs=[anywhere] * 6,
        out_specs=pl.BlockSpec(memory_space=pltpu.VMEM),
        scratch_shapes=[
            pltpu.VMEM((G, I * K, D), bf16),
            pltpu.VMEM((4, D, D), bf16),
            pltpu.VMEM((1, D), f32),
            pltpu.VMEM((G, I * K, D), bf16),
            pltpu.VMEM((G, I * K, D), bf16),
            pltpu.VMEM((line_of * 2 * G, I * K, D), bf16),
            pltpu.VMEM((N, D), f32),
            pltpu.VMEM((2 * N, D), f32),
            pltpu.VMEM((K, 2 * J, D), f32),
            pltpu.VMEM((2 * I * J, D), f32),
            pltpu.VMEM((N, D), f32),
            pltpu.VMEM((N, D), f32),
            pltpu.VMEM((line_of * G * 2, I * J, D), bf16),
            pltpu.VMEM((G, 2, rows_of, I * J, D), bf16),
            dma, dma, dma, dma, dma, dma((line_of * G,)), dma, dma((G,)),
            pltpu.SemaphoreType.REGULAR, pltpu.SemaphoreType.REGULAR((line_of - 1,)),
        ],
        compiler_params=pltpu.CompilerParams(collective_id=0, has_side_effects=True),
    )(pieces, left_weight, right_weight, mid_gain.reshape(1, -1), out_weight, out_gate)
    return jnp.transpose(update.reshape(J, K, D), (1, 0, 2))


def body(rows_of, columns_of, *arrays):
    K, J, D = arrays[0].shape
    fits = (
        columns_of == 2 * rows_of
        and columns_of == 8
        and K == 2 * J
        and arrays[1].shape == (D, D)
        and D % 128 == 0
        and J <= 16
        and J % PIECES == 0
    )
    if fits:
        return kernel_body(rows_of, columns_of // 2, *arrays)
    return plain_body(*arrays)


def solution(mesh):
    placed = (P("pr", "pc", None), P(), P(), P(), P(), P())
    return jax.shard_map(
        functools.partial(body, mesh.shape["pr"], mesh.shape["pc"]),
        mesh=mesh, in_specs=placed, out_specs=P("pr", "pc", None), check_vma=False,
    )
```

```python
import functools

import jax
import jax.numpy as jnp
from jax import lax
from jax.experimental import pallas as pl
from jax.experimental.pallas import tpu as pltpu
from jax.sharding import PartitionSpec as P

PIECES = 3
MESH = pl.DeviceIdType.MESH


def whole(*chips):
    return tuple((chip, g) for chip in chips for g in range(PIECES))


def mixed(*chips):
    return tuple((chip, g) for g in range(PIECES) for chip in chips)


FIRST = (
    (whole(1), whole(0, 2), whole(0, 1, 3), mixed(0, 2, 1)),
    ((), whole(0, 2), whole(1), mixed(0, 2, 1)),
)
UP = (((), whole(3), (), ()), (whole(1), (), whole(3), ()))
LATER = ((mixed(2, 3), (), (), ()), (mixed(2, 3), (), (), ()))
GREET = (
    (1, 1, 0, 0), (2, 1, 1, 0), (3, 1, 2, 0), (1, 1, 2, 1), (2, 1, 1, 1), (3, 1, 2, 1),
)
RISEN = (
    (1, 1, 0, 0, 2), (2, 1, 0, 0, 3), (2, 1, 1, 0, 3),
    (1, 0, 0, 1, 1), (2, 0, 0, 1, 2), (3, 0, 0, 1, 3), (3, 0, 2, 1, 3),
)
ORDER = (
    (whole(1) + mixed(3, 2), whole(0) + mixed(2, 3), whole(1, 0, 3), whole(2) + mixed(1, 0)),
    (whole(1) + mixed(2, 3), whole(0) + mixed(2, 3), whole(1, 0, 3), whole(2) + mixed(0, 1)),
)


def scale_channels(values, channel_gain):
    centred = values - jnp.mean(values, axis=-1, keepdims=True)
    return (
        centred
        * lax.rsqrt(jnp.mean(centred * centred, axis=-1, keepdims=True) + 1e-05)
        * channel_gain
    )


def project_pair(pair_in, left_weight, right_weight):
    left = jnp.einsum("ijc,cd->ijd", pair_in, left_weight, preferred_element_type=jnp.float32)
    right = jnp.einsum("ijc,cd->ijd", pair_in, right_weight, preferred_element_type=jnp.float32)
    return (pair_in, left.astype(jnp.bfloat16), right.astype(jnp.bfloat16))


def close_update(mixed, ready, mid_gain, out_weight, out_gate):
    scaled = scale_channels(mixed.astype(jnp.float32), mid_gain).astype(jnp.bfloat16)
    scaled = lax.optimization_barrier(scaled)
    gate = jax.nn.sigmoid(
        jnp.einsum("ijc,cd->ijd", ready, out_gate, preferred_element_type=jnp.float32)
    )
    return (
        jnp.einsum("ijd,dc->ijc", scaled, out_weight, preferred_element_type=jnp.float32) * gate
    ).astype(jnp.bfloat16)


def plain_body(pair_state, left_weight, right_weight, mid_gain, out_weight, out_gate):
    ready, left, right = project_pair(pair_state, left_weight, right_weight)
    count = pair_state.shape[0] * lax.axis_size("pr")
    left_lines, right_lines = (
        lax.all_to_all(left, "pr", split_axis=2, concat_axis=0, tiled=True),
        lax.all_to_all(right, "pr", split_axis=2, concat_axis=0, tiled=True),
    )
    strip = jnp.einsum(
        "kid,kjd->ijd",
        lax.all_gather(left_lines, "pc", axis=1, tiled=True),
        right_lines,
        preferred_element_type=jnp.float32,
    )
    strip = (strip * count ** (-0.5)).astype(jnp.bfloat16)
    mixed = lax.all_to_all(strip, "pr", split_axis=0, concat_axis=2, tiled=True)
    return close_update(mixed, ready, mid_gain, out_weight, out_gate)


def kernel(
    rows_of, line_of, J,
    x_hbm, wl_hbm, wr_hbm, gain_hbm, wo_hbm, wg_hbm, o_ref,
    xv, weights, gain, xsib, lv, zbuf, lbuf, rflat, rbuf, flat, merged, gate, pout, pin,
    x_in, weights_in, gain_in, x_recv, z_sent, z_recv, p_sent, p_recv, ready, risen,
):
    N, D = xv.shape[0] * xv.shape[1], xv.shape[2]
    K = N // J
    G = PIECES
    I = J // G
    part = I * J
    last = line_of - 1
    a = lax.axis_index("pr")
    c = lax.axis_index("pc")
    z, core = c // 2, c % 2
    other = 1 - core
    sib = 2 * z + other
    p, q = a % 2, a // 2
    across, along_y, opposite = a + 1 - 2 * p, (a + 2) % rows_of, rows_of - 1 - a
    inner = ((z + 1) % line_of) // 2
    relaying = inner * core

    def at_level(values):
        picked = values[0]
        for level in range(1, line_of):
            picked = picked + (z // level) * (1 - z // (level + 1)) * (values[level] - values[0])
        return picked

    def pick(lower, upper):
        return lower + core * (upper - lower)

    barrier = pltpu.get_barrier_semaphore()

    def tell(semaphore, row, column):
        pl.semaphore_signal(semaphore, inc=1, device_id=(row, column), device_id_type=MESH)

    def tell_chip(semaphore, row):
        tell(semaphore, row, c)
        tell(semaphore, row, sib)

    load = pltpu.make_async_copy(x_hbm, xv, x_in)
    load.start()
    for n, weight in enumerate((wl_hbm, wr_hbm, wg_hbm, wo_hbm)):
        pltpu.make_async_copy(weight, weights.at[n], weights_in).start()
    load_gain = pltpu.make_async_copy(gain_hbm, gain, gain_in)
    load_gain.start()

    tell(barrier, a, sib)
    for level in range(1, line_of):

        @pl.when(z < level)
        def _():
            tell(barrier, a, 2 * level + other)

    for level, half, target, end in GREET:

        @pl.when(jnp.logical_and(z == level, core == half))
        def _():
            tell(barrier, a, 2 * target + end)

    pl.when(p == 0)(lambda: tell_chip(barrier, across))
    pl.when(q == 0)(lambda: tell_chip(barrier, along_y))
    pl.when(a == 0)(lambda: tell_chip(barrier, opposite))

    routes = [
        [sorted({chip for chip, g in FIRST[h][l] + UP[h][l] + LATER[h][l]}) for l in range(line_of)]
        for h in range(2)
    ]

    def place(origin, half, g):
        return zbuf.at[(origin * 2 + half) * G + g]

    def along(src, origin, half, g, column, slot):
        return pltpu.make_async_remote_copy(
            src_ref=src, dst_ref=place(origin, half, g), send_sem=z_sent,
            recv_sem=z_recv.at[slot], device_id=(a, column), device_id_type=MESH,
        )

    def flow(half, level, target, g):
        held = half == 1 and 0 < level < last and 0 < target < last
        column = 2 * target + (1 if held else 1 - half)
        slot = (last if held else (level - target - 1) % line_of) * G + g
        return along(lv.at[g], level, half, g, column, slot)

    def everywhere(act):
        for half in range(2):
            for level in range(line_of):
                if act.keywords["plan"][half][level]:
                    pl.when(jnp.logical_and(z == level, core == half))(functools.partial(act, half, level))

    def launch(half, level, plan):
        seen = set()
        for target, g in plan[half][level]:
            if target not in seen and any(entry[2:] == (level, half, target) for entry in RISEN):
                pl.semaphore_wait(risen.at[target - 1], 1)
            seen.add(target)
            flow(half, level, target, g).start()

    def arrived(origin, half, g, slot):
        pltpu.make_async_copy(xv.at[0], place(origin, half, g), z_recv.at[slot]).wait()

    to_sib = pltpu.make_async_remote_copy(
        src_ref=xv, dst_ref=xsib, send_sem=z_sent, recv_sem=x_recv,
        device_id=(a, sib), device_id_type=MESH,
    )

    greeted = [
        [1 + l + sum(entry[2:] == (l, h) for entry in GREET) for h in range(2)] for l in range(line_of)
    ]
    lower, upper = (at_level([greeted[l][h] for l in range(line_of)]) for h in range(2))
    pl.semaphore_wait(barrier, pick(lower, upper) + 2 * (p + q + p * q))
    for level, half, target, end, chip in RISEN:

        @pl.when(jnp.logical_and(z == level, core == half))
        def _():
            tell(risen.at[chip - 1], a, 2 * target + end)

    pl.when(p == 1)(lambda: tell_chip(ready, across))
    pl.when(q == 1)(lambda: tell_chip(ready, along_y))
    pl.when(a == rows_of - 1)(lambda: tell_chip(ready, opposite))

    load.wait()
    to_sib.start()
    pltpu.make_async_copy(weights, weights, weights_in).wait()
    for g in range(G):
        rows = slice(g * I * K, (g + 1) * I * K)
        left = jnp.dot(xv[g], weights[0], preferred_element_type=jnp.float32)
        lv[g] = left.astype(lv.dtype)
        lbuf[rows, :] = left
    everywhere(functools.partial(launch, plan=FIRST))
    load_gain.wait()
    xs = xv[...].reshape(N, D)
    rflat[:N, :] = jnp.dot(xs, weights[1], preferred_element_type=jnp.float32)
    gate[...] = jax.nn.sigmoid(jnp.dot(xs, weights[2], preferred_element_type=jnp.float32))

    everywhere(functools.partial(launch, plan=UP))
    to_sib.wait_recv()
    rflat[N:, :] = jnp.dot(xsib[...].reshape(N, D), weights[1], preferred_element_type=jnp.float32)
    for k in range(K):
        rbuf[k] = rflat[pl.ds(k, 2 * J, stride=K), :]


    def contract(t, origin, half, g, base):
        def step(k, sums):
            right = rbuf[k]
            return tuple(
                total + lbuf[pl.ds(base + i * K + k, 1), :] * right for i, total in enumerate(sums)
            )

        sums = lax.fori_loop(
            0, K, step, tuple(jnp.zeros((2 * J, D), jnp.float32) for _ in range(I)), unroll=K
        )
        landing, sem = pin.at[g, half, a], p_recv.at[g]
        away = pltpu.make_async_remote_copy(
            src_ref=pout.at[2 * t], dst_ref=landing, send_sem=p_sent, recv_sem=sem,
            device_id=(origin, c), device_id_type=MESH,
        )
        stay = pltpu.make_async_copy(pout.at[2 * t], landing, sem)
        side = pltpu.make_async_remote_copy(
            src_ref=pout.at[2 * t + 1], dst_ref=landing, send_sem=p_sent, recv_sem=sem,
            device_id=(origin, sib), device_id_type=MESH,
        )
        for i in range(I):
            flat[i * J : (i + 1) * J, :] = sums[i][:J]
            flat[part + i * J : part + (i + 1) * J, :] = sums[i][J:]
        pout[2 * t] = flat[:part, :].astype(pout.dtype)
        pl.when(origin != a)(away.start)
        pl.when(origin == a)(stay.start)
        pout[2 * t + 1] = flat[part:, :].astype(pout.dtype)
        side.start()

    @pl.when(a < rows_of - 1)
    def _():
        pl.semaphore_wait(ready, 2 * ((1 - p) + (1 - q) + (1 - p) * (1 - q)))

    for g in range(G):
        contract(g, z, core, g, g * I * K)

    everywhere(functools.partial(launch, plan=LATER))

    peer = last - z
    outer = (peer + 2) % line_of
    relays = []
    for g in range(G):
        held = place(peer, 1, g)
        relays.append(along(held, peer, 1, g, 2 * outer, G + g))
        relays.append(along(held, peer, 1, g, sib, (peer - z + last) % line_of * G + g))

    @pl.when(relaying == 1)
    def _():
        for g in range(G):
            arrived(peer, 1, g, last * G + g)
            for copy in relays[2 * g : 2 * g + 2]:
                copy.start()

    for n in range(last * G):
        origin, g = (
            pick(*(at_level([ORDER[half][level][n][e] for level in range(line_of)]) for half in range(2)))
            for e in range(2)
        )
        arrived(origin, other, g, (origin - z + last) % line_of * G + g)
        lbuf[: I * K, :] = zbuf[(origin * 2 + other) * G + g].astype(jnp.float32)
        contract(G + n, origin, other, g, 0)

    for g in range(G):
        for ahead in ([0] if g == 0 else range(1, G) if g == 1 else []):
            pltpu.make_async_copy(pin.at[ahead], pin.at[ahead], p_recv.at[ahead]).wait()
        totals = []
        for s in range(2):
            total = pin[g, s, 0].astype(jnp.float32)
            for row in range(1, rows_of):
                total += pin[g, s, row].astype(jnp.float32)
            totals.append(total)
        total = jnp.concatenate(totals, axis=0) * (K * rows_of) ** (-0.5)
        total = total.astype(jnp.bfloat16).astype(jnp.float32)
        scaled = scale_channels(total, gain[...]).astype(jnp.bfloat16)
        out = jnp.dot(scaled, weights[3], preferred_element_type=jnp.float32)
        for s in range(2):
            for i in range(I):
                first_row = s * part + i * J
                merged[pl.ds((s * G + g) * I + i, J, stride=K), :] = out[first_row : first_row + J]
    o_ref[...] = (merged[...] * gate[...]).astype(o_ref.dtype)

    def settle(half, level, plan):
        sends = (len(plan[half][level]) + 1) * G
        held = [s for s in plan[half][level] if half == 1 and 0 < level < last and 0 < s < last]
        sent = zbuf.at[pl.ds(0, sends + 2 * G * len(held))]
        pltpu.make_async_copy(sent, sent, z_sent).wait()

    everywhere(functools.partial(settle, plan=routes))
    sent = pout.at[pl.ds(0, (2 * line_of - 1) * G)]
    pltpu.make_async_copy(sent, sent, p_sent).wait()


def kernel_body(rows_of, line_of, pair_state, left_weight, right_weight, mid_gain, out_weight, out_gate):
    K, J, D = pair_state.shape
    N = K * J
    G = PIECES
    I = J // G
    f32, bf16 = jnp.float32, jnp.bfloat16
    anywhere = pl.BlockSpec(memory_space=pl.ANY)
    dma = pltpu.SemaphoreType.DMA
    pieces = jnp.transpose(pair_state, (1, 0, 2)).reshape(G, I * K, D)
    update = pl.pallas_call(
        functools.partial(kernel, rows_of, line_of, J),
        out_shape=pltpu.VMEM((N, D), bf16),
        in_specs=[anywhere] * 6,
        out_specs=pl.BlockSpec(memory_space=pltpu.VMEM),
        scratch_shapes=[
            pltpu.VMEM((G, I * K, D), bf16),
            pltpu.VMEM((4, D, D), bf16),
            pltpu.VMEM((1, D), f32),
            pltpu.VMEM((G, I * K, D), bf16),
            pltpu.VMEM((G, I * K, D), bf16),
            pltpu.VMEM((line_of * 2 * G, I * K, D), bf16),
            pltpu.VMEM((N, D), f32),
            pltpu.VMEM((2 * N, D), f32),
            pltpu.VMEM((K, 2 * J, D), f32),
            pltpu.VMEM((2 * I * J, D), f32),
            pltpu.VMEM((N, D), f32),
            pltpu.VMEM((N, D), f32),
            pltpu.VMEM((line_of * G * 2, I * J, D), bf16),
            pltpu.VMEM((G, 2, rows_of, I * J, D), bf16),
            dma, dma, dma, dma, dma, dma((line_of * G,)), dma, dma((G,)),
            pltpu.SemaphoreType.REGULAR, pltpu.SemaphoreType.REGULAR((line_of - 1,)),
        ],
        compiler_params=pltpu.CompilerParams(collective_id=0, has_side_effects=True),
    )(pieces, left_weight, right_weight, mid_gain.reshape(1, -1), out_weight, out_gate)
    return jnp.transpose(update.reshape(J, K, D), (1, 0, 2))


def body(rows_of, columns_of, *arrays):
    K, J, D = arrays[0].shape
    fits = (
        columns_of == 2 * rows_of
        and columns_of == 8
        and K == 2 * J
        and arrays[1].shape == (D, D)
        and D % 128 == 0
        and J <= 16
        and J % PIECES == 0
    )
    if fits:
        return kernel_body(rows_of, columns_of // 2, *arrays)
    return plain_body(*arrays)


def solution(mesh):
    placed = (P("pr", "pc", None), P(), P(), P(), P(), P())
    return jax.shard_map(
        functools.partial(body, mesh.shape["pr"], mesh.shape["pc"]),
        mesh=mesh, in_specs=placed, out_specs=P("pr", "pc", None), check_vma=False,
    )
```

```python
import functools

import jax
import jax.numpy as jnp
from jax import lax
from jax.experimental import pallas as pl
from jax.experimental.pallas import tpu as pltpu
from jax.sharding import PartitionSpec as P

PIECES = 3
MESH = pl.DeviceIdType.MESH


def whole(*chips):
    return tuple((chip, g) for chip in chips for g in range(PIECES))


def mixed(*chips):
    return tuple((chip, g) for g in range(PIECES) for chip in chips)


FIRST = (
    (whole(1), whole(0, 2), whole(0, 1, 3), mixed(0, 2, 1)),
    ((), whole(0, 2), whole(1), mixed(0, 2, 1)),
)
UP = (((), whole(3), (), ()), (whole(1), (), whole(3), ()))
LATER = ((mixed(2, 3), (), (), ()), (mixed(2, 3), (), (), ()))
GREET = (
    (1, 1, 0, 0), (2, 1, 1, 0), (3, 1, 2, 0), (1, 1, 2, 1), (2, 1, 1, 1), (3, 1, 2, 1),
)
RISEN = (
    (1, 1, 0, 0, 2), (2, 1, 0, 0, 3), (2, 1, 1, 0, 3),
    (1, 0, 0, 1, 1), (2, 0, 0, 1, 2), (3, 0, 0, 1, 3), (3, 0, 2, 1, 3),
)
ORDER = (
    (whole(1) + mixed(3, 2), whole(0) + mixed(2, 3), whole(1, 0, 3), whole(2) + mixed(1, 0)),
    (whole(1) + mixed(2, 3), whole(0) + mixed(3, 2), whole(1, 0, 3), whole(2) + mixed(0, 1)),
)


def scale_channels(values, channel_gain):
    centred = values - jnp.mean(values, axis=-1, keepdims=True)
    return (
        centred
        * lax.rsqrt(jnp.mean(centred * centred, axis=-1, keepdims=True) + 1e-05)
        * channel_gain
    )


def project_pair(pair_in, left_weight, right_weight):
    left = jnp.einsum("ijc,cd->ijd", pair_in, left_weight, preferred_element_type=jnp.float32)
    right = jnp.einsum("ijc,cd->ijd", pair_in, right_weight, preferred_element_type=jnp.float32)
    return (pair_in, left.astype(jnp.bfloat16), right.astype(jnp.bfloat16))


def close_update(mixed, ready, mid_gain, out_weight, out_gate):
    scaled = scale_channels(mixed.astype(jnp.float32), mid_gain).astype(jnp.bfloat16)
    scaled = lax.optimization_barrier(scaled)
    gate = jax.nn.sigmoid(
        jnp.einsum("ijc,cd->ijd", ready, out_gate, preferred_element_type=jnp.float32)
    )
    return (
        jnp.einsum("ijd,dc->ijc", scaled, out_weight, preferred_element_type=jnp.float32) * gate
    ).astype(jnp.bfloat16)


def plain_body(pair_state, left_weight, right_weight, mid_gain, out_weight, out_gate):
    ready, left, right = project_pair(pair_state, left_weight, right_weight)
    count = pair_state.shape[0] * lax.axis_size("pr")
    left_lines, right_lines = (
        lax.all_to_all(left, "pr", split_axis=2, concat_axis=0, tiled=True),
        lax.all_to_all(right, "pr", split_axis=2, concat_axis=0, tiled=True),
    )
    strip = jnp.einsum(
        "kid,kjd->ijd",
        lax.all_gather(left_lines, "pc", axis=1, tiled=True),
        right_lines,
        preferred_element_type=jnp.float32,
    )
    strip = (strip * count ** (-0.5)).astype(jnp.bfloat16)
    mixed = lax.all_to_all(strip, "pr", split_axis=0, concat_axis=2, tiled=True)
    return close_update(mixed, ready, mid_gain, out_weight, out_gate)


def kernel(
    rows_of, line_of, J,
    x_hbm, wl_hbm, wr_hbm, gain_hbm, wo_hbm, wg_hbm, o_ref,
    xv, weights, gain, xsib, lv, zbuf, lbuf, rflat, rbuf, flat, merged, gate, pout, pin,
    x_recv, z_sent, z_recv, p_sent, p_recv, ready, risen,
):
    N, D = xv.shape[0] * xv.shape[1], xv.shape[2]
    K = N // J
    G = PIECES
    I = J // G
    part = I * J
    last = line_of - 1
    a = lax.axis_index("pr")
    c = lax.axis_index("pc")
    z, core = c // 2, c % 2
    other = 1 - core
    sib = 2 * z + other
    p, q = a % 2, a // 2
    across, along_y, opposite = a + 1 - 2 * p, (a + 2) % rows_of, rows_of - 1 - a
    inner = ((z + 1) % line_of) // 2
    relaying = inner * core

    def at_level(values):
        picked = values[0]
        for level in range(1, line_of):
            picked = picked + (z // level) * (1 - z // (level + 1)) * (values[level] - values[0])
        return picked

    def pick(lower, upper):
        return lower + core * (upper - lower)

    barrier = pltpu.get_barrier_semaphore()

    def tell(semaphore, row, column):
        pl.semaphore_signal(semaphore, inc=1, device_id=(row, column), device_id_type=MESH)

    def tell_chip(semaphore, row):
        tell(semaphore, row, c)
        tell(semaphore, row, sib)

    load = pltpu.make_async_copy(x_hbm, xv, z_sent)
    load.start()
    for n, weight in enumerate((wl_hbm, wr_hbm, wg_hbm, wo_hbm)):
        pltpu.make_async_copy(weight, weights.at[n], p_sent).start()
    load_gain = pltpu.make_async_copy(gain_hbm, gain, p_sent)

    tell(barrier, a, sib)
    for level in range(1, line_of):

        @pl.when(z < level)
        def _():
            tell(barrier, a, 2 * level + other)

    for level, half, target, end in GREET:

        @pl.when(jnp.logical_and(z == level, core == half))
        def _():
            tell(barrier, a, 2 * target + end)

    pl.when(p == 0)(lambda: tell_chip(barrier, across))
    pl.when(q == 0)(lambda: tell_chip(barrier, along_y))
    pl.when(a == 0)(lambda: tell_chip(barrier, opposite))

    routes = [
        [sorted({chip for chip, g in FIRST[h][l] + UP[h][l] + LATER[h][l]}) for l in range(line_of)]
        for h in range(2)
    ]

    def place(origin, half, g):
        return zbuf.at[(origin * 2 + half) * G + g]

    def along(src, origin, half, g, column, slot):
        return pltpu.make_async_remote_copy(
            src_ref=src, dst_ref=place(origin, half, g), send_sem=z_sent,
            recv_sem=z_recv.at[slot], device_id=(a, column), device_id_type=MESH,
        )

    def flow(half, level, target, g):
        held = half == 1 and 0 < level < last and 0 < target < last
        column = 2 * target + (1 if held else 1 - half)
        slot = (last if held else (level - target - 1) % line_of) * G + g
        return along(lv.at[g], level, half, g, column, slot)

    def everywhere(act):
        for half in range(2):
            for level in range(line_of):
                if act.keywords["plan"][half][level]:
                    pl.when(jnp.logical_and(z == level, core == half))(functools.partial(act, half, level))

    def launch(half, level, plan):
        seen = set()
        for target, g in plan[half][level]:
            if target not in seen and any(entry[2:] == (level, half, target) for entry in RISEN):
                pl.semaphore_wait(risen.at[target - 1], 1)
            seen.add(target)
            flow(half, level, target, g).start()

    def arrived(origin, half, g, slot):
        pltpu.make_async_copy(xv.at[0], place(origin, half, g), z_recv.at[slot]).wait()

    to_sib = pltpu.make_async_remote_copy(
        src_ref=xv, dst_ref=xsib, send_sem=z_sent, recv_sem=x_recv,
        device_id=(a, sib), device_id_type=MESH,
    )

    greeted = [
        [1 + l + sum(entry[2:] == (l, h) for entry in GREET) for h in range(2)] for l in range(line_of)
    ]
    lower, upper = (at_level([greeted[l][h] for l in range(line_of)]) for h in range(2))
    pl.semaphore_wait(barrier, pick(lower, upper) + 2 * (p + q + p * q))
    for level, half, target, end, chip in RISEN:

        @pl.when(jnp.logical_and(z == level, core == half))
        def _():
            tell(risen.at[chip - 1], a, 2 * target + end)

    pl.when(p == 1)(lambda: tell_chip(ready, across))
    pl.when(q == 1)(lambda: tell_chip(ready, along_y))
    pl.when(a == rows_of - 1)(lambda: tell_chip(ready, opposite))

    load.wait()
    to_sib.start()
    pltpu.make_async_copy(weights, weights, p_sent).wait()
    load_gain.start()
    xs = xv[...].reshape(N, D)
    left = jnp.dot(xs, weights[0], preferred_element_type=jnp.float32)
    lv[...] = left.astype(lv.dtype).reshape(lv.shape)
    everywhere(functools.partial(launch, plan=FIRST))
    lbuf[...] = left
    rflat[:N, :] = jnp.dot(xs, weights[1], preferred_element_type=jnp.float32)
    gate[...] = jax.nn.sigmoid(jnp.dot(xs, weights[2], preferred_element_type=jnp.float32))

    everywhere(functools.partial(launch, plan=UP))
    to_sib.wait_recv()
    load_gain.wait()
    rflat[N:, :] = jnp.dot(xsib[...].reshape(N, D), weights[1], preferred_element_type=jnp.float32)
    for k in range(K):
        rbuf[k] = rflat[pl.ds(k, 2 * J, stride=K), :]


    def contract(t, origin, half, g, base):
        def step(k, sums):
            right = rbuf[k]
            return tuple(
                total + lbuf[pl.ds(base + i * K + k, 1), :] * right for i, total in enumerate(sums)
            )

        sums = lax.fori_loop(
            0, K, step, tuple(jnp.zeros((2 * J, D), jnp.float32) for _ in range(I)), unroll=K
        )
        landing, sem = pin.at[g, half, a], p_recv.at[g]
        away = pltpu.make_async_remote_copy(
            src_ref=pout.at[2 * t], dst_ref=landing, send_sem=p_sent, recv_sem=sem,
            device_id=(origin, c), device_id_type=MESH,
        )
        stay = pltpu.make_async_copy(pout.at[2 * t], landing, sem)
        side = pltpu.make_async_remote_copy(
            src_ref=pout.at[2 * t + 1], dst_ref=landing, send_sem=p_sent, recv_sem=sem,
            device_id=(origin, sib), device_id_type=MESH,
        )
        for i in range(I):
            flat[i * J : (i + 1) * J, :] = sums[i][:J]
            flat[part + i * J : part + (i + 1) * J, :] = sums[i][J:]
        pout[2 * t] = flat[:part, :].astype(pout.dtype)
        pl.when(origin != a)(away.start)
        pl.when(origin == a)(stay.start)
        pout[2 * t + 1] = flat[part:, :].astype(pout.dtype)
        side.start()

    @pl.when(a < rows_of - 1)
    def _():
        pl.semaphore_wait(ready, 2 * ((1 - p) + (1 - q) + (1 - p) * (1 - q)))

    for g in range(G):
        contract(g, z, core, g, g * I * K)

    everywhere(functools.partial(launch, plan=LATER))

    peer = last - z
    outer = (peer + 2) % line_of
    relays = []
    for g in range(G):
        held = place(peer, 1, g)
        relays.append(along(held, peer, 1, g, 2 * outer, G + g))
        relays.append(along(held, peer, 1, g, sib, (peer - z + last) % line_of * G + g))

    @pl.when(relaying == 1)
    def _():
        for g in range(G):
            arrived(peer, 1, g, last * G + g)
            for copy in relays[2 * g : 2 * g + 2]:
                copy.start()

    for n in range(last * G):
        origin, g = (
            pick(*(at_level([ORDER[half][level][n][e] for level in range(line_of)]) for half in range(2)))
            for e in range(2)
        )
        arrived(origin, other, g, (origin - z + last) % line_of * G + g)
        lbuf[: I * K, :] = zbuf[(origin * 2 + other) * G + g].astype(jnp.float32)
        contract(G + n, origin, other, g, 0)

    for g in range(G):
        for ahead in ([0] if g == 0 else range(1, G) if g == 1 else []):
            pltpu.make_async_copy(pin.at[ahead], pin.at[ahead], p_recv.at[ahead]).wait()
        totals = []
        for s in range(2):
            total = pin[g, s, 0].astype(jnp.float32)
            for row in range(1, rows_of):
                total += pin[g, s, row].astype(jnp.float32)
            totals.append(total)
        total = jnp.concatenate(totals, axis=0) * (K * rows_of) ** (-0.5)
        total = total.astype(jnp.bfloat16).astype(jnp.float32)
        scaled = scale_channels(total, gain[...]).astype(jnp.bfloat16)
        out = jnp.dot(scaled, weights[3], preferred_element_type=jnp.float32)
        for s in range(2):
            for i in range(I):
                first_row = s * part + i * J
                merged[pl.ds((s * G + g) * I + i, J, stride=K), :] = out[first_row : first_row + J]
    o_ref[...] = (merged[...] * gate[...]).astype(o_ref.dtype)

    def settle(half, level, plan):
        sends = (len(plan[half][level]) + 1) * G
        held = [s for s in plan[half][level] if half == 1 and 0 < level < last and 0 < s < last]
        sent = zbuf.at[pl.ds(0, sends + 2 * G * len(held))]
        pltpu.make_async_copy(sent, sent, z_sent).wait()

    everywhere(functools.partial(settle, plan=routes))
    sent = pout.at[pl.ds(0, (2 * line_of - 1) * G)]
    pltpu.make_async_copy(sent, sent, p_sent).wait()


def kernel_body(rows_of, line_of, pair_state, left_weight, right_weight, mid_gain, out_weight, out_gate):
    K, J, D = pair_state.shape
    N = K * J
    G = PIECES
    I = J // G
    f32, bf16 = jnp.float32, jnp.bfloat16
    anywhere = pl.BlockSpec(memory_space=pl.ANY)
    dma = pltpu.SemaphoreType.DMA
    pieces = jnp.transpose(pair_state, (1, 0, 2)).reshape(G, I * K, D)
    update = pl.pallas_call(
        functools.partial(kernel, rows_of, line_of, J),
        out_shape=pltpu.VMEM((N, D), bf16),
        in_specs=[anywhere] * 6,
        out_specs=pl.BlockSpec(memory_space=pltpu.VMEM),
        scratch_shapes=[
            pltpu.VMEM((G, I * K, D), bf16),
            pltpu.VMEM((4, D, D), bf16),
            pltpu.VMEM((1, D), f32),
            pltpu.VMEM((G, I * K, D), bf16),
            pltpu.VMEM((G, I * K, D), bf16),
            pltpu.VMEM((line_of * 2 * G, I * K, D), bf16),
            pltpu.VMEM((N, D), f32),
            pltpu.VMEM((2 * N, D), f32),
            pltpu.VMEM((K, 2 * J, D), f32),
            pltpu.VMEM((2 * I * J, D), f32),
            pltpu.VMEM((N, D), f32),
            pltpu.VMEM((N, D), f32),
            pltpu.VMEM((line_of * G * 2, I * J, D), bf16),
            pltpu.VMEM((G, 2, rows_of, I * J, D), bf16),
            dma, dma, dma((line_of * G,)), dma, dma((G,)),
            pltpu.SemaphoreType.REGULAR, pltpu.SemaphoreType.REGULAR((line_of - 1,)),
        ],
        compiler_params=pltpu.CompilerParams(collective_id=0, has_side_effects=True),
    )(pieces, left_weight, right_weight, mid_gain.reshape(1, -1), out_weight, out_gate)
    return jnp.transpose(update.reshape(J, K, D), (1, 0, 2))


def body(rows_of, columns_of, *arrays):
    K, J, D = arrays[0].shape
    fits = (
        columns_of == 2 * rows_of
        and columns_of == 8
        and K == 2 * J
        and arrays[1].shape == (D, D)
        and D % 128 == 0
        and J <= 16
        and J % PIECES == 0
    )
    if fits:
        return kernel_body(rows_of, columns_of // 2, *arrays)
    return plain_body(*arrays)


def solution(mesh):
    placed = (P("pr", "pc", None), P(), P(), P(), P(), P())
    return jax.shard_map(
        functools.partial(body, mesh.shape["pr"], mesh.shape["pc"]),
        mesh=mesh, in_specs=placed, out_specs=P("pr", "pc", None), check_vma=False,
    )
```
